512 devices in a mesh: grp: 8 (over y_lo, x), shard: 64 (over z, y_hi, core).
Axes of the slice: x: 4, y: 4 (y_hi: 2, y_lo: 2; y = y_hi * 2 + y_lo), z: 16, core: 2. Of those that a mesh axis runs over, the one named last changes fastest.
Arguments:
- window: bfloat16 [128, 4096], P('grp'), may hold values from -6 to 6
- weight: bfloat16 [11008, 4096], P('shard'), may hold values from -0.09375 to 0.09375
- factor_a: bfloat16 [1024, 4, 4096], P(('grp', 'shard')), may hold values from -6 to 6
- factor_b: bfloat16 [1024, 4, 11008], P(('grp', 'shard')), may hold values from -6 to 6
- fitness: float32 [1024], P(('grp', 'shard')), may hold values from -4 to 4
Outputs:
- perturbed: bfloat16 [11008, 16384], P('shard', 'grp')
- update: float32 [11008, 4096], P('shard', 'grp')
The draws below stay inside these ranges and needn't reach their ends.
All inputs are finite; a program needn't handle non-finite values.
Results may differ from the reference program's by a relative error of at most 0.0029.
Values may be sent and summed in bfloat16 or wider, within the bound.
A program may use at most 64 MiB of HBM per device.

```python
import math
import jax
import jax.numpy as jnp
from jax import lax

D = 4096
FF = 11008
TOK = 16
RANK = 4
CANDS = 1024
N_GRP = 8


def levels(rng, extent, split, smallest, high):
    def one(dim, blocks):
        draws = jax.random.uniform(jax.random.fold_in(jax.random.fold_in(rng, 6), dim), (blocks,), jnp.float32, smallest / len(split), high / len(split))
        return jnp.repeat(jnp.exp(draws), extent[dim] // blocks).reshape((-1,) + (1,) * (len(extent) - dim - 1))

    level = one(*split[0])
    for cut in split[1:]:
        level = level * one(*cut)
    return level


def normal_values(own_key, shape, width, most, pieces=(), kind=jnp.bfloat16):
    gain = levels(own_key, shape, pieces, -0.22, 0.18) if pieces else 1.0
    values = jax.random.normal(own_key, shape, jnp.float32) * width * gain
    return jnp.minimum(jnp.maximum(values, -most), most).astype(kind)


def setup_inputs(seed: int = 0) -> dict:
    streams_of = jax.random.split(jax.random.key(seed), 6)
    window = normal_values(streams_of[0], (N_GRP * TOK, D), 1.0, 6.0, ((0, 8),))
    weight = normal_values(streams_of[1], (FF, D), D ** -0.5, 0.09375, ((0, 64),))
    factor_a = normal_values(streams_of[2], (CANDS, RANK, D), 1.0, 6.0, ((0, 512),))
    factor_b = normal_values(streams_of[3], (CANDS, RANK, FF), 1.0, 6.0, ((0, 512),))
    fitness = normal_values(streams_of[4], (CANDS,), 1.0, 4.0, ((0, 512),), jnp.float32)
    return {"window": window, "weight": weight, "factor_a": factor_a, "factor_b": factor_b, "fitness": fitness}


def reference(window, weight, factor_a, factor_b, fitness):
    total_cands = factor_a.shape[0]
    group_count = window.shape[0] // TOK
    per_group = total_cands // group_count
    perturb = 0.25 / math.sqrt(D)
    base_out = jnp.dot(window, weight.T, preferred_element_type=jnp.float32).reshape(group_count, TOK, FF)
    x_groups = window.reshape(group_count, TOK, D)
    a_groups = factor_a.reshape(group_count, per_group, RANK, D)
    b_groups = factor_b.reshape(group_count, per_group, RANK, FF)

    def one_group(inputs):
        group_window, group_a, group_b, group_base = inputs
        projected = jnp.einsum('td,crd->crt', group_window.astype(jnp.float32), group_a.astype(jnp.float32), precision=lax.Precision.HIGHEST)
        low_rank = jnp.einsum('crt,crf->ctf', projected, group_b.astype(jnp.float32), precision=lax.Precision.HIGHEST)
        return (group_base[None] + perturb * low_rank).astype(jnp.bfloat16)
    perturbed = lax.map(one_group, (x_groups, a_groups, b_groups, base_out)).reshape(total_cands * TOK, FF).T
    weighted = (fitness[:, None, None] * factor_b.astype(jnp.float32)).astype(jnp.bfloat16)
    update = jnp.dot(weighted.reshape(total_cands * RANK, FF).T, factor_a.reshape(total_cands * RANK, D), preferred_element_type=jnp.float32)
    update = update * (0.5 / math.sqrt(total_cands))
    return (perturbed, update)
```

```python
import functools
import math

import jax
import jax.numpy as jnp
from jax import lax
from jax.experimental import pallas as pl
from jax.experimental.pallas import tpu as pltpu
from jax.sharding import Mesh
from jax.sharding import PartitionSpec as P

AXES = ("gy", "gx", "z", "yh", "core")
GRP = ("gy", "gx")
SHARD = ("z", "yh", "core")
MESH = pl.DeviceIdType.MESH
F32 = jnp.float32
BF16 = jnp.bfloat16
NZ, NG, NX = 16, 8, 4
ROWS = 8
WIDE = 768
OWN = 172
TAIL = OWN - 128
TAILPAD = 48


def remote(src, dst, ssem, rsem, **where):
    return pltpu.make_async_remote_copy(
        src_ref=src, dst_ref=dst, send_sem=ssem, recv_sem=rsem, device_id=where, device_id_type=MESH
    )


def dot_tn(left, right):
    return lax.dot_general(left, right, (((0,), (0,)), ((), ())), preferred_element_type=F32)


def dot_nt(left, right):
    return lax.dot_general(left, right, (((1,), (1,)), ((), ())), preferred_element_type=F32)


def columns_at(b_ref, start, at):
    width = b_ref.shape[1]
    base = min(start // 128 * 128, width - 256)
    pair = b_ref[:, base : base + 256].astype(F32)
    turn = (at - (start - base)) % 256
    if turn:
        pair = pltpu.roll(pair, turn, 1)
    return pair[:, :128]


def kernel(
    perturb, step_scale,
    fit_ref, win_ref, a_ref, b_ref, w_ref,
    pert_ref, upd_ref,
    wrep, bsend, ball, aall, bpert, wmat, amat, ubuf, basebuf, rs1, rs2s, rs2r,
    a1s, a1r, b1s, b1r, rgs, rgr, gxs, gxr, pxs, pxr, r1s, r1r, r2s, r2r,
):
    gy, gx, z, yh, core = (lax.axis_index(name) for name in AXES)
    g = gy * NX + gx
    ogy, oyh, ocore = 1 - gy, 1 - yh, 1 - core
    right, left = lax.rem(z + 1, NZ), lax.rem(z + NZ - 1, NZ)
    xr, xl, xo = lax.rem(gx + 1, NX), lax.rem(gx + 3, NX), lax.rem(gx + 2, NX)

    barrier = pltpu.get_barrier_semaphore()

    def greet(**where):
        pl.semaphore_signal(barrier, inc=1, device_id=where, device_id_type=MESH)

    for o in range(1, NZ):
        greet(z=lax.rem(z + o, NZ))
    for o in range(1, NG):
        p = lax.rem(g + o, NG)
        greet(gy=p // NX, gx=lax.rem(p, NX))
    greet(core=ocore)
    greet(yh=oyh)
    greet(yh=oyh, core=ocore)

    for k in range(8):
        wrep[16 * k : 16 * k + 16, :] = win_ref[...]
    proj = dot_nt(a_ref[...], wrep[...])
    high = proj.astype(BF16).astype(F32)
    low = proj - high
    lane = lax.broadcasted_iota(jnp.int32, (ROWS, 128), 1)
    row = lax.broadcasted_iota(jnp.int32, (ROWS, 128), 0)
    fit = jnp.where(row < ROWS // 2, fit_ref[0], fit_ref[1])
    fit0 = fit.astype(BF16).astype(F32)
    rest = fit - fit0
    fit1 = rest.astype(BF16).astype(F32)
    fit2 = rest - fit1
    extra = jnp.where(
        lane >= 112,
        low,
        jnp.where(lane >= 48, high, jnp.where(lane == 44, fit0, jnp.where(lane == 45, fit1, fit2))),
    )
    for k in range(NZ):
        first = 4 * OWN * k
        for j in range(4):
            bsend[k, :, 128 * j : 128 * j + 128] = columns_at(b_ref, first + OWN * j, 0).astype(BF16)
        for half in range(2):
            lo = columns_at(b_ref, first + OWN * (2 * half) + 128, 0)
            hi = columns_at(b_ref, first + OWN * (2 * half + 1) + 128, 64)
            tile = jnp.where(lane < TAIL, lo, jnp.where((lane >= 64) & (lane < 64 + TAIL), hi, extra))
            bsend[k, :, 512 + 128 * half : 640 + 128 * half] = tile.astype(BF16)
    mine = pl.ds(pl.multiple_of(g * 512, 512), 512)
    aall[z, g] = a_ref[:, mine]
    ball[gy, gx, z] = bsend[z]

    pl.semaphore_wait(barrier, NZ - 1 + NG - 1 + 3)

    a1 = []
    for o in range(1, NG):
        p = lax.rem(g + o, NG)
        cols = pl.ds(pl.multiple_of(p * 512, 512), 512)
        a1.append(
            remote(a_ref.at[:, cols], aall.at[z, g], a1s.at[o], a1r.at[o], gy=p // NX, gx=lax.rem(p, NX))
        )
        a1[-1].start()
    b1 = []
    for o in (8, 7, 9, 6, 10, 5, 11, 4, 12, 3, 13, 2, 14, 1, 15):
        p = lax.rem(z + o, NZ)
        b1.append(remote(bsend.at[p], ball.at[gy, gx, z], b1s.at[o], b1r.at[o], z=p))
        b1[-1].start()

    def a1_wait(o):
        p = lax.rem(g + NG - o, NG)
        remote(aall.at[z, p], aall.at[z, p], a1s.at[o], a1r.at[o], core=ocore).wait_recv()

    for o in range(1, NG):
        a1_wait(o)

    def ring(way, step, half):
        src = lax.rem(z + NZ - (step - 1), NZ) if way == 0 else lax.rem(z + step - 1, NZ)
        part = aall.at[src, pl.ds(4 * half, 4)]
        k = (way, step - 1, half)
        return remote(part, part, rgs.at[k], rgr.at[k], z=right if way == 0 else left)

    def ring_recv(way, step, half):
        src = lax.rem(z + NZ - step, NZ) if way == 0 else lax.rem(z + step, NZ)
        part = aall.at[src, pl.ds(4 * half, 4)]
        k = (way, step - 1, half)
        remote(part, part, rgs.at[k], rgr.at[k], z=right if way == 0 else left).wait_recv()

    def ring_has(way, step, half):
        return step < 8 or way == half

    def ring_go(step):
        for half in range(2):
            for way in range(2):
                if step > 1:
                    ring_recv(way, step - 1, half)
                if step < 9 and ring_has(way, step, half):
                    ring(way, step, half).start()

    ring_go(1)

    basebuf[...] = dot_nt(w_ref[...], wrep[...])

    ring_go(2)
    ring_go(3)

    for o in (1, 15, 2, 14, 3, 13, 4, 12, 5, 11, 6, 10, 7, 9, 8):
        p = lax.rem(z + NZ - o, NZ)
        remote(ball.at[gy, gx, p], ball.at[gy, gx, p], b1s.at[o], b1r.at[o], core=ocore).wait_recv()

    def gather(k, sy, sx, half, dest):
        part = ball.at[sy, sx, pl.ds(8 * half, 8)]
        return remote(part, part, gxs.at[k], gxr.at[k], **dest)

    sends = []

    def send(k, sy, sx, half, **dest):
        cp = gather(k, sy, sx, half, dest)
        cp.start()
        sends.append(cp)

    def got(k, sy, sx, half):
        gather(k, sy, sx, half, {"core": ocore}).wait_recv()

    for half in range(2):
        send(half, gy, gx, half, gy=ogy)
    for half in range(2):
        send(2 + half, gy, gx, half, gx=xr)
        send(4 + half, gy, gx, half, gx=xl)

    me = yh * 2 + core
    px = []
    for o, (py, pc) in enumerate(((yh, ocore), (oyh, core), (oyh, ocore))):
        main = pl.ds(pl.multiple_of((py * 2 + pc) * 128, 128), 128)
        tail = pl.ds(pl.multiple_of(512 + py * 128, 128), 128)
        for t, (lanes, at) in enumerate(((main, 0), (tail, 128))):
            px.append(
                remote(
                    ball.at[gy, gx, :, :, lanes], bpert.at[:, me, :, pl.ds(at, 128)],
                    pxs.at[o, t], pxr.at[o, t], yh=py, core=pc,
                )
            )
            px[-1].start()
    bpert[:, me, :, 0:128] = ball[gy, gx, :, :, pl.ds(pl.multiple_of(me * 128, 128), 128)]
    bpert[:, me, :, 128:256] = ball[gy, gx, :, :, pl.ds(pl.multiple_of(512 + yh * 128, 128), 128)]

    ring_go(4)
    ring_go(5)
    for half in range(2):
        got(half, ogy, gx, half)
    for half in range(2):
        send(6 + half, ogy, gx, half, gx=xr)
        send(8 + half, ogy, gx, half, gx=xl)
    got(2, gy, xl, 0)
    send(10, gy, xl, 0, gx=xr)
    got(5, gy, xr, 1)
    send(11, gy, xr, 1, gx=xl)
    ring_go(6)
    got(6, ogy, xl, 0)
    send(12, ogy, xl, 0, gx=xr)
    got(9, ogy, xr, 1)
    send(13, ogy, xr, 1, gx=xl)
    ring_go(7)

    for o, (py, pc) in enumerate(((yh, ocore), (oyh, core), (oyh, ocore))):
        for t in range(2):
            part = bpert.at[:, py * 2 + pc, :, pl.ds(128 * t, 128)]
            remote(part, part, pxs.at[o, t], pxr.at[o, t], core=ocore).wait_recv()
    lane_in = lax.broadcasted_iota(jnp.int32, (128, 128), 0)
    lane_out = lax.broadcasted_iota(jnp.int32, (128, 128), 1)
    pick_hi = (lane_in == 48 + lane_out % 16).astype(F32).astype(BF16)
    pick_lo = (lane_in == 112 + lane_out % 16).astype(F32).astype(BF16)
    pick_fit = ((lane_in >= 44) & (lane_in < 47)).astype(F32).astype(BF16)
    crow = lax.broadcasted_iota(jnp.int32, (128, 512), 0) // 4
    ccol = lax.broadcasted_iota(jnp.int32, (128, 512), 1) // 16
    same = crow == ccol

    def perturb_block(k, _):
        packets = bpert[pl.ds(4 * k, 4)].astype(F32).reshape(128, 256).astype(BF16)
        tail = packets[:, 128:]
        hi = jnp.dot(tail, pick_hi, preferred_element_type=F32)
        lo = jnp.dot(tail, pick_lo, preferred_element_type=F32)
        hi = jnp.where(same, jnp.concatenate([hi] * 4, axis=1), 0.0).astype(BF16)
        lo = jnp.where(same, jnp.concatenate([lo] * 4, axis=1), 0.0).astype(BF16)
        acc = dot_tn(packets, hi) + dot_tn(packets, lo)
        base = jnp.concatenate([basebuf[...]] * 4, axis=1)
        cols = pl.ds(pl.multiple_of(k * 512, 512), 512)
        pert_ref[0:128, cols] = (base[0:128] + perturb * acc[0:128]).astype(BF16)
        rem = jnp.where(core == 0, acc[128 : 128 + TAILPAD], acc[192 : 192 + TAILPAD])
        pert_ref[128:OWN, cols] = (base[128:OWN] + perturb * rem[:TAIL]).astype(BF16)
        return 0

    lax.fori_loop(0, 4, perturb_block, 0)

    ring_go(8)
    for k, sy, sx, half in (
        (3, gy, xl, 1), (4, gy, xr, 0), (7, ogy, xl, 1), (8, ogy, xr, 0),
        (10, gy, xo, 0), (11, gy, xo, 1), (12, ogy, xo, 0), (13, ogy, xo, 1),
    ):
        got(k, sy, sx, half)

    def weigh(p, _):
        packets = ball[p // NX, lax.rem(p, NX)].astype(F32).reshape(128, WIDE)
        fits = jnp.dot(packets[:, 512:640].astype(BF16), pick_fit, preferred_element_type=F32)
        fits = jnp.concatenate([fits] * 6, axis=1)
        wmat[pl.ds(pl.multiple_of(p * 128, 128), 128), :] = (packets * fits).astype(BF16)
        return 0

    lax.fori_loop(0, NG, weigh, 0)

    for way in range(2):
        ring_recv(way, 8, way)

    def flatten(p, _):
        rows = aall[:, p].astype(F32).reshape(128, 512)
        amat[pl.ds(pl.multiple_of(p * 128, 128), 128), :] = rows.astype(BF16)
        return 0

    lax.fori_loop(0, NG, flatten, 0)

    def product(k, _):
        rows = pl.ds(pl.multiple_of(k * 128, 128), 128)
        ubuf[rows, :] = dot_tn(wmat[:, rows], amat[...])
        return 0

    lax.fori_loop(0, 6, product, 0)

    def main_rows(py, pc):
        return pl.ds(pl.multiple_of((py * 2 + pc) * 128, 128), 128)

    def tail_rows(py, pc):
        return pl.ds(pl.multiple_of(512 + (py * 2 + pc) * 64, 64), TAILPAD)

    first = []
    for k, py in enumerate((oyh, yh)):
        first.append(
            remote(ubuf.at[main_rows(py, ocore)], rs1.at[k, pl.ds(0, 128)], r1s.at[k, 0], r1r.at[k, 0], core=ocore)
        )
        first.append(
            remote(ubuf.at[tail_rows(py, ocore)], rs1.at[k, pl.ds(128, TAILPAD)], r1s.at[k, 1], r1r.at[k, 1], core=ocore)
        )
    for cp in first:
        cp.start()
    first[0].wait_recv()
    first[1].wait_recv()
    rs2s[0:128, :] = ubuf[main_rows(oyh, core), :] + rs1[0, 0:128, :]
    rs2s[128:176, :] = ubuf[tail_rows(oyh, core), :] + rs1[0, 128:176, :]
    second = remote(rs2s, rs2r, r2s, r2r, yh=oyh)
    second.start()
    first[2].wait_recv()
    first[3].wait_recv()
    rs1[1, 0:128, :] = ubuf[main_rows(yh, core), :] + rs1[1, 0:128, :]
    rs1[1, 128:176, :] = ubuf[tail_rows(yh, core), :] + rs1[1, 128:176, :]
    second.wait_recv()
    upd_ref[...] = (rs1[1, 0:OWN, :] + rs2r[0:OWN, :]) * step_scale

    for cp in a1 + b1 + sends + px + first + [second]:
        cp.wait_send()
    for step in range(1, 9):
        for half in range(2):
            for way in range(2):
                if ring_has(way, step, half):
                    ring(way, step, half).wait_send()


def local(window, weight, factor_a, factor_b, fitness):
    d_model = window.shape[1]
    total = factor_a.shape[0] * NZ * 4 * NG
    perturb = 0.25 / math.sqrt(d_model)
    step_scale = 0.5 / math.sqrt(total)
    a8 = factor_a.reshape(ROWS, d_model)
    b8 = factor_b.reshape(ROWS, factor_b.shape[2])
    vmem = pl.BlockSpec(memory_space=pltpu.VMEM)
    dma = pltpu.SemaphoreType.DMA
    return pl.pallas_call(
        functools.partial(kernel, perturb, step_scale),
        name="es_step",
        out_shape=(
            jax.ShapeDtypeStruct((OWN, NZ * 128), BF16),
            jax.ShapeDtypeStruct((OWN, 512), F32),
        ),
        in_specs=[pl.BlockSpec(memory_space=pltpu.SMEM)] + [vmem] * 4,
        out_specs=(vmem, vmem),
        scratch_shapes=[
            pltpu.VMEM((128, d_model), BF16),
            pltpu.VMEM((NZ, ROWS, WIDE), BF16),
            pltpu.VMEM((2, NX, NZ, ROWS, WIDE), BF16),
            pltpu.VMEM((NZ, NG, ROWS, 512), BF16),
            pltpu.VMEM((NZ, 4, ROWS, 256), BF16),
            pltpu.VMEM((1024, WIDE), BF16),
            pltpu.VMEM((1024, 512), BF16),
            pltpu.VMEM((WIDE, 512), F32),
            pltpu.VMEM((OWN, 128), F32),
            pltpu.VMEM((2, 128 + TAILPAD, 512), F32),
            pltpu.VMEM((128 + TAILPAD, 512), F32),
            pltpu.VMEM((128 + TAILPAD, 512), F32),
            dma((NG,)), dma((NG,)), dma((NZ,)), dma((NZ,)),
            dma((2, 8, 2)), dma((2, 8, 2)), dma((14,)), dma((14,)),
            dma((3, 2)), dma((3, 2)), dma((2, 2)), dma((2, 2)), dma, dma,
        ],
        compiler_params=pltpu.CompilerParams(
            collective_id=0, has_side_effects=True, vmem_limit_bytes=48 * 1024 * 1024
        ),
    )(fitness, window, a8, b8, weight)


def solution(mesh):
    split = Mesh(mesh.devices.reshape(2, NX, NZ, 2, 2), AXES)
    return jax.shard_map(
        local,
        mesh=split,
        in_specs=(P(GRP, None), P(SHARD, None), P(GRP + SHARD, None, None), P(GRP + SHARD, None, None), P(GRP + SHARD)),
        out_specs=(P(SHARD, GRP), P(SHARD, GRP)),
        check_vma=False,
    )
```
